32 devices in a mesh: cfg: 2 (over core), tp: 4 (over y, x), dp: 4 (over z).
Axes of the slice: x: 2, y: 2, z: 4, core: 2. Of those that a mesh axis runs over, the one named last changes fastest.
Arguments:
- hidden_in: bfloat16 [2, 128, 2048], P('cfg', 'dp', 'tp'), may hold values from -6 to 6
- attn_gain: float32 [2048], replicated, may hold values from 0.25 to 1.75
- w_qkv: bfloat16 [2048, 3, 2048], P(None, None, 'tp'), may hold values from -3 to 3
- w_out: bfloat16 [2048, 2048], P('tp'), may hold values from -0.125 to 0.125
- cache_keys: bfloat16 [2, 128, 128, 2048], P('cfg', 'dp', None, 'tp'), may hold values from -11 to 11
- cache_values: bfloat16 [2, 128, 128, 2048], P('cfg', 'dp', None, 'tp'), may hold values from -6 to 6
- cache_len: int32 [128], P('dp'), may hold values from 33 to 128
- text_len: int32 [128], P('dp'), may hold values from 1 to 31
- final_gain: float32 [2048], replicated, may hold values from 0.25 to 1.75
- lm_head: bfloat16 [4, 2048, 2048], P(None, 'dp', 'tp'), may hold values from -12 to 12
- guidance: float32 [128], P('dp'), may hold values from 1.5 to 4
- uniforms: float32 [128, 4, 2048], P('dp', 'cfg', 'tp'), may hold values from 1e-06 to 0.999999
Outputs:
- sample_logprobs: float32 [128, 4, 2048], P('dp', 'cfg', 'tp')
- residual_out: bfloat16 [2, 128, 2048], P('cfg', 'dp', 'tp')
The draws below stay inside these ranges and needn't reach their ends.
Inputs may be any that keep to these rules, and one draw needn't show every extreme that they name: text_len of a stream is below its cache_len.
All inputs are finite; a program needn't handle non-finite values.
Results may differ from the reference program's by a relative error of at most 0.0023.
The reference program's roundings to bfloat16 on the way (of `tokens_norm`, `projections`, `weights`, `attended` and `normed`) count: a program that leaves them out, or rounds other values in their place, can miss the bound.
Values may be sent and summed in bfloat16 or wider, within the bound.
A program may use at most 64 MiB of HBM per device.

```python
import math
import jax
import jax.numpy as jnp
from jax import lax

D = 2048
HEADS = 32
HEAD_DIM = 64
CB = 4
VOCAB = 2048
CACHE = 128
STREAMS = 128


def shared_pattern(key):
    base = jax.random.fold_in(key, 7001)
    pattern = jnp.clip(jax.random.normal(jax.random.fold_in(base, 1), (D,), jnp.float32), -2.0, 2.0)
    directions = jnp.clip(jax.random.normal(jax.random.fold_in(base, 2), (HEADS, HEAD_DIM), jnp.float32), -2.0, 2.0)
    stream_order = jax.random.permutation(jax.random.fold_in(base, 3), STREAMS)
    chosen = stream_order < max(STREAMS // 8, 1)
    stream_lift = jax.random.uniform(jax.random.fold_in(base, 4), (STREAMS,), jnp.float32, 0.4, 0.95)
    strength = jnp.where(chosen, stream_lift, 0.0)
    head_order = jax.random.permutation(jax.random.fold_in(base, 5), HEADS)
    head_lift = jax.random.uniform(jax.random.fold_in(base, 6), (HEADS,), jnp.float32, 0.3, 1.3)
    head_strength = jnp.where(head_order < HEADS // 2, head_lift, 0.0)
    return (pattern, directions, strength, head_strength)


def unit_noise(key, shape):
    return jnp.clip(jax.random.normal(key, shape, jnp.float32), -6.0, 6.0)


def draw_hidden_in(key, part):
    pattern, directions, strength, head_strength = shared_pattern(key)
    noise = unit_noise(jax.random.fold_in(key, 11), (2, STREAMS, D))
    lift = strength[None, :, None]
    rows = 2.5 * lift * pattern[None, None, :] + jnp.sqrt(1.0 - lift * lift) * noise
    return jnp.clip(rows, -6.0, 6.0).astype(jnp.bfloat16)


def draw_w_qkv(key, part):
    pattern, directions, strength, head_strength = shared_pattern(key)
    noise = jnp.clip(unit_noise(jax.random.fold_in(key, 21), (D, 3, HEADS * HEAD_DIM)), -4.0, 4.0) / math.sqrt(D)
    spike = (20.0 / D * head_strength[:, None] * directions).reshape(HEADS * HEAD_DIM)
    query_part = pattern[:, None] * spike[None, :]
    slot_mask = (jnp.arange(3) == 0).astype(jnp.float32)
    whole = noise + query_part[:, None, :] * slot_mask[None, :, None]
    return jnp.clip(whole, -3.0, 3.0).astype(jnp.bfloat16)


def draw_cache_keys(key, part):
    pattern, directions, strength, head_strength = shared_pattern(key)
    noise = unit_noise(jax.random.fold_in(key, 31), (2, STREAMS, CACHE, HEADS * HEAD_DIM))
    reach = 20.0 / math.sqrt(HEAD_DIM)
    apart = 1.008
    positions = jnp.arange(CACHE)
    at_first = positions == CACHE // 4 - 1
    at_second = positions == CACHE // 4
    factor = jnp.where(at_first, reach, jnp.where(at_second, reach * apart, 0.0))
    marked = at_first | at_second
    flat_dir = directions.reshape(HEADS * HEAD_DIM)
    aligned = factor[:, None] * flat_dir[None, :]
    keys = jnp.where(marked[None, None, :, None], aligned[None, None, :, :] + 0.05 * noise, noise)
    return jnp.clip(keys, -11.0, 11.0).astype(jnp.bfloat16)


def draw_lm_head(key, part):
    pattern, directions, strength, head_strength = shared_pattern(key)
    noise = jnp.clip(unit_noise(jax.random.fold_in(key, 41), (CB, D, VOCAB)), -4.0, 4.0) / math.sqrt(D)
    chosen = jnp.stack([jax.random.permutation(jax.random.fold_in(key, 50 + codebook), VOCAB) < 8 for codebook in range(CB)])
    code_lift = jax.random.uniform(jax.random.fold_in(key, 42), (CB, VOCAB), jnp.float32, 0.94, 1.0)
    alpha = jnp.where(chosen, 360.0 / D * code_lift, 0.0)
    whole = noise + alpha[:, None, :] * pattern[None, :, None]
    return jnp.clip(whole, -12.0, 12.0).astype(jnp.bfloat16)


def plant(values, key, smallest, high):
    dims = values.shape
    index_at = [jax.random.randint(jax.random.fold_in(key, axis), (), 0, dims[axis]) for axis in range(len(dims))]
    values = values.at[tuple(index_at)].set(smallest)
    longest = dims.index(max(dims))
    index_at[longest] = (index_at[longest] + 1) % dims[longest]
    return values.at[tuple(index_at)].set(high)


def levels(key, extent, shards, least, high):
    gain, own = 1.0, jax.random.fold_in(key, 6)
    for axis_at, parts in shards:
        heights = jnp.exp(jax.random.uniform(jax.random.fold_in(own, axis_at), (parts,), jnp.float32, least / len(shards), high / len(shards)))
        gain = gain * jnp.repeat(heights, extent[axis_at] // parts).reshape([-1 if axis == axis_at else 1 for axis in range(len(extent))])
    return gain


def bell_draw(stream_key, extent, width, most, split=(), kind=jnp.bfloat16):
    entries = width * jax.random.normal(stream_key, extent, jnp.float32)
    if split:
        entries = entries * levels(stream_key, extent, split, -0.22, 0.18)
    return jnp.clip(entries, -most, most).astype(kind)


def setup_inputs(seed: int = 0) -> dict:
    key_list = jax.random.split(jax.random.key(seed), 13)
    return {
        "hidden_in": draw_hidden_in(jax.random.fold_in(key_list[12], 71), 0),
        "attn_gain": jnp.clip(1.0 + 0.15 * jax.random.normal(key_list[1], (D,), jnp.float32), 0.25, 1.75),
        "w_qkv": draw_w_qkv(jax.random.fold_in(key_list[12], 71), 0),
        "w_out": bell_draw(key_list[3], (HEADS * HEAD_DIM, D), (HEADS * HEAD_DIM) ** -0.5, 0.125, ((0, 4),)),
        "cache_keys": draw_cache_keys(jax.random.fold_in(key_list[12], 71), 0),
        "cache_values": bell_draw(key_list[5], (2, STREAMS, CACHE, HEADS * HEAD_DIM), 1.0, 6.0, ((0, 2), (1, 4), (3, 4))),
        "cache_len": plant(jax.random.randint(key_list[6], (STREAMS,), CACHE // 4 + 1, CACHE + 1), jax.random.fold_in(key_list[6], 1), CACHE // 4 + 1, CACHE).astype(jnp.int32),
        "text_len": plant(jax.random.randint(key_list[7], (STREAMS,), 1, CACHE // 4), jax.random.fold_in(key_list[7], 1), 1, (CACHE // 4) - 1).astype(jnp.int32),
        "final_gain": jnp.clip(1.0 + 0.15 * jax.random.normal(key_list[8], (D,), jnp.float32), 0.25, 1.75),
        "lm_head": draw_lm_head(jax.random.fold_in(key_list[12], 71), 0),
        "guidance": jnp.clip(1.5 + 2.5 * jax.random.uniform(key_list[10], (STREAMS,), jnp.float32) ** levels(key_list[10], (STREAMS,), ((0, 4),), -0.2, 0.2), 1.5, 4.0),
        "uniforms": jnp.clip(9.999999974752427e-07 + 0.999998 * jax.random.uniform(key_list[11], (STREAMS, CB, VOCAB), jnp.float32) ** levels(key_list[11], (STREAMS, CB, VOCAB), ((0, 4), (1, 2), (2, 4)), -0.2, 0.2), 9.999999974752427e-07, 0.999999),
    }


epsilon = 1e-05
far_below = -1e+30

def layer_norm(values_in, gain_vec):
    average = lax.optimization_barrier(jnp.mean(values_in, axis=-1, keepdims=True))
    spread = lax.optimization_barrier(jnp.mean((values_in - average) ** 2, axis=-1, keepdims=True))
    return (values_in - average) * lax.rsqrt(spread + epsilon) * gain_vec

def reference(hidden_in, attn_gain, w_qkv, w_out, cache_keys, cache_values, cache_len, text_len, final_gain, lm_head, guidance, uniforms):
    positions = jnp.arange(CACHE, dtype=jnp.int32)
    inv_root = 1.0 / HEAD_DIM ** 0.5
    residuals = []
    logit_list = []
    for branch in range(2):
        tokens_in = hidden_in[branch].astype(jnp.float32)
        tokens_norm = layer_norm(tokens_in, attn_gain).astype(jnp.bfloat16)
        projections = jnp.dot(tokens_norm, w_qkv.reshape(D, 3 * HEADS * HEAD_DIM), preferred_element_type=jnp.float32)
        projections = projections.astype(jnp.bfloat16).reshape(STREAMS, 3, HEADS, HEAD_DIM).astype(jnp.float32)
        queries = projections[:, 0]
        new_keys = projections[:, 1]
        new_values = projections[:, 2]
        key_rows = cache_keys[branch].astype(jnp.float32).reshape(STREAMS, CACHE, HEADS, HEAD_DIM)
        scores = jnp.einsum('shd,sjhd->shj', queries, key_rows) * inv_root
        usable = positions[None, :] < cache_len[:, None]
        if branch == 1:
            usable = usable & (positions[None, :] >= text_len[:, None])
        scores = jnp.where(usable[:, None, :], scores, far_below)
        self_score = lax.optimization_barrier(jnp.sum(queries * new_keys, axis=-1)) * inv_root
        peak = jnp.maximum(lax.optimization_barrier(jnp.max(scores, axis=-1)), self_score)
        raw_weights = jnp.exp(scores - peak[..., None])
        self_raw = jnp.exp(self_score - peak)
        denom = lax.optimization_barrier(jnp.sum(raw_weights, axis=-1)) + self_raw
        weights = (raw_weights / denom[..., None]).astype(jnp.bfloat16).astype(jnp.float32)
        self_weight = (self_raw / denom).astype(jnp.bfloat16).astype(jnp.float32)
        value_rows = cache_values[branch].astype(jnp.float32).reshape(STREAMS, CACHE, HEADS, HEAD_DIM)
        attended = jnp.einsum('shj,sjhd->shd', weights, value_rows) + self_weight[..., None] * new_values
        attended = attended.astype(jnp.bfloat16).reshape(STREAMS, HEADS * HEAD_DIM)
        projected = jnp.dot(attended, w_out, preferred_element_type=jnp.float32)
        residual = (tokens_in + projected).astype(jnp.bfloat16)
        residuals.append(residual)
        normed = layer_norm(residual.astype(jnp.float32), final_gain).astype(jnp.bfloat16)
        logits = jnp.einsum('sd,cdv->scv', normed.astype(jnp.float32), lm_head.astype(jnp.float32))
        logit_list.append(logits)
    conditioned = logit_list[0]
    unconditioned = logit_list[1]
    guided = unconditioned + guidance[:, None, None] * (conditioned - unconditioned)
    perturbed = guided - jnp.log(-jnp.log(uniforms))
    peak_code = lax.optimization_barrier(jnp.max(perturbed, axis=-1, keepdims=True))
    log_total = jnp.log(lax.optimization_barrier(jnp.sum(jnp.exp(perturbed - peak_code), axis=-1, keepdims=True))) + peak_code
    return (perturbed - log_total, jnp.stack(residuals))
```

```python
import functools
import math

import jax
import jax.numpy as jnp
from jax import lax
from jax.experimental import pallas as pl
from jax.experimental.pallas import tpu as pltpu
from jax.sharding import PartitionSpec as P

HEAD_DIM = 64
EPS = 1e-05
FAR_BELOW = -1e30
MESH = pl.DeviceIdType.MESH
F32 = jnp.float32
BF16 = jnp.bfloat16


def norm_scale(blocks, features):
    average = sum(jnp.sum(block, axis=-1, keepdims=True) for block in blocks) / features
    spread = sum(
        jnp.sum((block - average) ** 2, axis=-1, keepdims=True) for block in blocks
    )
    return average, lax.rsqrt(spread / features + EPS)


def grid_peers(t, T):
    X = math.isqrt(T)
    X = X if X * X == T else T
    Y = T // X
    y, x = t // X, lax.rem(t, X)
    shifts = [(dy, dx) for dy in range(Y) for dx in range(X) if (dy, dx) != (0, 0)]
    shifts.sort(key=lambda shift: -((shift[0] > 0) + (shift[1] > 0)))
    return [
        (dy * X + dx, lax.rem(y + dy, Y) * X + lax.rem(x + dx, X)) for dy, dx in shifts
    ]


def line_peers(d, Dp):
    peers = []
    for k in range(Dp - 1):
        down = Dp - 1 - k
        down = jnp.where(down > d, down, down - 1)
        up = jnp.where(k < d, k, k + 1)
        peers.append(jnp.where(d < Dp // 2, down, up))
    return peers


def kernel(
    hid_h, ag_h, w_h, wo_h, k_h, v_h, cl_h, tl_h, fg_h, lm_h, gd_h, un_h,
    out_ref, res_ref,
    cl_ref, tl_ref, gd_ref,
    xg, ag_ref, fg_ref, nrm, w, kc, vc, wo, lm, un,
    q, nk, nv, sc, ss, att, part, rs, rg, nrm2, nz, gz, lp, rz, own, swap, gb, pt, pk, st,
    lsem, xs, xr, ps, pr, gs, gr, zs, zr, hs, hr, ls, lr, os, orr, ts, tr,
):
    c = lax.axis_index("cfg")
    t = lax.axis_index("tp")
    d = lax.axis_index("dp")
    T, S, F = xg.shape
    Dp, rows2, G = nz.shape
    Hs = S // 2
    D = T * F
    H = F // HEAD_DIM
    CB, _, V = lm.shape
    CBH = CB // 2
    CACHE = kc.shape[1]
    t_peers = grid_peers(t, T)
    z_peers = line_peers(d, Dp)

    barrier = pltpu.get_barrier_semaphore()
    cores = (c, 1 - c)
    for _, peer in t_peers:
        for core in cores:
            pl.semaphore_signal(
                barrier, inc=1, device_id={"tp": peer, "cfg": core}, device_id_type=MESH
            )
    for peer in z_peers:
        for core in cores:
            pl.semaphore_signal(
                barrier, inc=1, device_id={"dp": peer, "cfg": core}, device_id_type=MESH
            )
    pl.semaphore_signal(barrier, inc=1, device_id={"cfg": 1 - c}, device_id_type=MESH)

    count = 0

    def load(src, dst):
        nonlocal count
        copy = pltpu.make_async_copy(src, dst, lsem.at[count])
        count += 1
        copy.start()
        return copy

    hid = load(hid_h.at[0], xg.at[t])
    load_ag = load(ag_h, ag_ref)
    load_fg = load(fg_h, fg_ref)
    load_gd = load(gd_h, gd_ref)
    load_cl = load(cl_h, cl_ref)
    load_tl = load(tl_h, tl_ref)
    loads = {"w": [], "k": [], "v": []}
    for slot in range(3):
        loads["w"].append(load(w_h.at[slot], w.at[slot]))
    quarter = S // 4
    for piece in range(4):
        rows = pl.ds(piece * quarter, quarter)
        loads["k"].append(load(k_h.at[0, rows], kc.at[rows]))
    for piece in range(4):
        rows = pl.ds(piece * quarter, quarter)
        loads["v"].append(load(v_h.at[0, rows], vc.at[rows]))
    load_wo = load(wo_h, wo)
    load_un = load(un_h, un)
    load_lm = load(lm_h, lm)

    pl.semaphore_wait(barrier, 2 * (T - 1) + 2 * (Dp - 1) + 1)

    def send(src, dst, send_sem, recv_sem, device):
        copy = pltpu.make_async_remote_copy(
            src_ref=src, dst_ref=dst, send_sem=send_sem, recv_sem=recv_sem,
            device_id=device, device_id_type=MESH,
        )
        copy.start()
        return copy

    def arrive(dst, recv_sem):
        pltpu.make_async_remote_copy(
            src_ref=dst, dst_ref=dst, send_sem=recv_sem, recv_sem=recv_sem,
            device_id={"cfg": 1 - c}, device_id_type=MESH,
        ).wait_recv()

    hid.wait()
    hid_sends = [
        send(xg.at[t], xg.at[t], xs.at[slot], xr.at[slot], {"tp": peer})
        for slot, peer in t_peers
    ]

    load_gd.wait()
    first = pl.multiple_of(c * Hs, Hs)
    other = pl.multiple_of((1 - c) * Hs, Hs)

    def fill(s, carry):
        gz[d, pl.ds(s, 1), :] = jnp.full((1, 128), gd_ref[first + s], F32)
        return carry

    lax.fori_loop(0, Hs, fill, 0)
    guide_sends = [
        send(gz.at[d], gz.at[d], hs.at[k], hr.at[d], {"dp": peer})
        for k, peer in enumerate(z_peers)
    ]

    load_ag.wait()
    load_fg.wait()
    load_cl.wait()
    load_tl.wait()
    for copy in hid_sends:
        copy.wait_recv()
    blocks = [xg[i].astype(F32) for i in range(T)]
    average, scale = norm_scale(blocks, D)
    for i in range(T):
        cols = slice(i * F, (i + 1) * F)
        nrm[:, cols] = ((blocks[i] - average) * scale * ag_ref[:, cols]).astype(BF16)

    for slot, dst in enumerate((q, nk, nv)):
        loads["w"][slot].wait()
        dst[...] = (
            jnp.dot(nrm[...], w[slot], preferred_element_type=F32).astype(BF16).astype(F32)
        )

    inv_root = 1.0 / HEAD_DIM**0.5
    own_head = (
        lax.broadcasted_iota(jnp.int32, (H, F), 1) // HEAD_DIM
        == lax.broadcasted_iota(jnp.int32, (H, F), 0)
    )
    positions = lax.broadcasted_iota(jnp.int32, (H, CACHE), 1)
    branch_low = jnp.where(c == 0, 0, 1)

    for copy in loads["k"]:
        copy.wait()

    def score_step(s, carry):
        spread = jnp.where(own_head, jnp.broadcast_to(q[pl.ds(s, 1), :], (H, F)), 0.0)
        raw = lax.dot_general(
            spread.astype(BF16), kc[s], (((1,), (1,)), ((), ())), preferred_element_type=F32
        )
        usable = (positions < cl_ref[s]) & (positions >= tl_ref[s] * branch_low)
        sc[s] = jnp.where(usable, raw * inv_root, FAR_BELOW)
        own_score = jnp.sum(spread * nk[pl.ds(s, 1), :], axis=-1, keepdims=True) * inv_root
        ss[s] = jnp.broadcast_to(own_score, (H, CACHE))
        return carry

    lax.fori_loop(0, S, score_step, 0, unroll=min(16, S))

    scores = sc[...]
    own_scores = ss[...]
    peak = jnp.maximum(jnp.max(scores, axis=-1, keepdims=True), own_scores)
    raw = jnp.exp(scores - peak)
    own_raw = jnp.exp(own_scores - peak)
    denom = jnp.sum(raw, axis=-1, keepdims=True) + own_raw
    sc[...] = raw / denom
    ss[...] = (own_raw / denom).astype(BF16).astype(F32)

    for copy in loads["v"]:
        copy.wait()

    def value_step(s, carry):
        mixed = jnp.dot(sc[s].astype(BF16), vc[s], preferred_element_type=F32)
        mixed = mixed + ss[s][:, 0:1] * nv[pl.ds(s, 1), :]
        att[pl.ds(s, 1), :] = jnp.sum(jnp.where(own_head, mixed, 0.0), axis=0, keepdims=True)
        return carry

    lax.fori_loop(0, S, value_step, 0, unroll=min(16, S))

    load_wo.wait()
    heads = att[...].astype(BF16)
    part_sends = []
    for slot, peer in t_peers:
        cols = pl.ds(pl.multiple_of(peer * F, 128), F)
        part[slot] = jnp.dot(heads, wo[:, cols], preferred_element_type=F32).astype(part.dtype)
        part_sends.append(
            send(part.at[slot], rs.at[slot], ps.at[slot], pr.at[slot], {"tp": peer})
        )
    cols = pl.ds(pl.multiple_of(t * F, 128), F)
    total = jnp.dot(heads, wo[:, cols], preferred_element_type=F32)
    total = xg[t].astype(F32) + total
    for copy, (slot, _) in reversed(list(zip(part_sends, t_peers))):
        copy.wait_recv()
        total = total + rs[slot].astype(F32)
    res_ref[0] = total.astype(BF16)
    branch_rows = pl.ds(pl.multiple_of(c * Hs, Hs), Hs)
    rg[t, branch_rows, :] = res_ref[0, pl.ds(first, Hs), :]
    res_sends = []
    mine, theirs = pl.ds(first, Hs), pl.ds(other, Hs)
    for slot, peer in t_peers:
        for side, (core, rows) in enumerate(((1 - c, theirs), (c, mine))):
            res_sends.append(
                send(
                    res_ref.at[0, rows], rg.at[t, branch_rows],
                    gs.at[slot, side], gr.at[slot, side], {"tp": peer, "cfg": core},
                )
            )
    res_sends.append(
        send(res_ref.at[0, theirs], rg.at[t, branch_rows], gs.at[0, 0], gr.at[0, 0], {"cfg": 1 - c})
    )

    load_un.wait()
    for book in range(CBH):
        gb[book] = jnp.log(-jnp.log(un[:, book, :]))

    for copy in res_sends:
        copy.wait_recv()
    blocks = [rg[i].astype(F32) for i in range(T)]
    average, scale = norm_scale(blocks, D)
    for i in range(T):
        cols = slice(i * F, (i + 1) * F)
        nrm2[:, cols] = ((blocks[i] - average) * scale * fg_ref[:, cols]).astype(BF16)

    norm_sends = []
    for k, peer in enumerate(z_peers):
        cols = pl.ds(pl.multiple_of(peer * G, 128), G)
        norm_sends.append(
            send(nrm2.at[:, cols], nz.at[d], zs.at[k], zr.at[d], {"dp": peer})
        )
    load_lm.wait()
    for peer in z_peers:
        arrive(gz.at[peer], hr.at[peer])

    def guided_block(source, both_rows, book):
        logits = jnp.dot(both_rows, lm[book], preferred_element_type=F32)
        cond, plain = logits[:Hs], logits[Hs:]
        return plain + gz[source][:, 0:1] * (cond - plain)

    cols = pl.ds(pl.multiple_of(d * G, 128), G)
    both_rows = nrm2[:, cols]
    own_sends = []
    for j in range(CBH):
        swap[j] = guided_block(d, both_rows, (1 - c) * CBH + j)
        own_sends.append(
            send(swap.at[j], own.at[c, j], os.at[j], orr.at[j], {"cfg": 1 - c})
        )
    for j in range(CBH):
        own[c, j] = guided_block(d, both_rows, c * CBH + j)
    logit_sends = []
    for k, peer in enumerate(z_peers):
        arrive(nz.at[peer], zr.at[peer])
        both_rows = nz[peer]
        for side, core in enumerate((1 - c, c)):
            for j in range(CBH):
                lp[k, side, j] = guided_block(peer, both_rows, core * CBH + j).astype(BF16)
                logit_sends.append(
                    send(
                        lp.at[k, side, j], rz.at[d, side, j],
                        ls.at[k, side, j], lr.at[d, side, j], {"dp": peer, "cfg": core},
                    )
                )
    lanes = lax.broadcasted_iota(jnp.int32, (Hs, 128), 1)
    for side, half in ((1, c), (0, 1 - c)):
        rows = pl.ds(pl.multiple_of(half * Hs, Hs), Hs)
        packed = jnp.zeros((Hs, 128), F32)
        for j in range(CBH):
            if side == 0:
                own_sends[j].wait_recv()
            total = own[half, j] - gb[j, rows, :]
            for peer in z_peers:
                arrive(rz.at[peer, side, j], lr.at[peer, side, j])
                total = total + rz[peer, side, j].astype(F32)
            peak = jnp.max(total, axis=-1, keepdims=True)
            mass = jnp.sum(jnp.exp(total - peak), axis=-1, keepdims=True)
            packed = jnp.where(lanes == 2 * j, peak, packed)
            packed = jnp.where(lanes == 2 * j + 1, mass, packed)
            pt[j, rows, :] = total
        pk[rows, :] = packed
    st[0] = jnp.transpose(pk[...])[:8]
    stat_sends = [
        send(st.at[0], st.at[slot], ts.at[slot], tr.at[slot], {"tp": peer})
        for slot, peer in t_peers
    ]
    for copy in stat_sends:
        copy.wait_recv()
    levels = lax.broadcasted_iota(jnp.int32, (8, S), 0)
    logs = jnp.zeros((8, S), F32)
    for j in range(CBH):
        peaks = [st[i, 2 * j : 2 * j + 1, :] for i in range(T)]
        masses = [st[i, 2 * j + 1 : 2 * j + 2, :] for i in range(T)]
        top = functools.reduce(jnp.maximum, peaks)
        mass = sum(m * jnp.exp(p - top) for p, m in zip(peaks, masses))
        logs = jnp.where(levels == j, jnp.log(mass) + top, logs)
    logs = jnp.transpose(logs)
    for j in range(CBH):
        out_ref[:, j, :] = pt[j] - logs[:, j : j + 1]

    for group in (
        hid_sends, guide_sends, part_sends, res_sends, norm_sends, own_sends,
        logit_sends, stat_sends,
    ):
        for copy in group:
            copy.wait_send()


def body(
    T, Dp,
    hidden_in, attn_gain, w_qkv, w_out, cache_keys, cache_values, cache_len, text_len,
    final_gain, lm_head, guidance, uniforms,
):
    _, S, F = hidden_in.shape
    D = attn_gain.shape[0]
    books, G, V = lm_head.shape
    CBH = uniforms.shape[1]
    CACHE = cache_keys.shape[2]
    H = F // HEAD_DIM
    Hs = S // 2
    anyspace = pl.BlockSpec(memory_space=pl.ANY)
    vmem = pl.BlockSpec(memory_space=pltpu.VMEM)
    dma = pltpu.SemaphoreType.DMA
    return pl.pallas_call(
        kernel,
        out_shape=(pltpu.VMEM((S, CBH, V), F32), pltpu.VMEM((1, S, F), BF16)),
        in_specs=[anyspace] * 12,
        out_specs=(vmem, vmem),
        scratch_shapes=[
            pltpu.SMEM((S,), jnp.int32),
            pltpu.SMEM((S,), jnp.int32),
            pltpu.SMEM((S,), F32),
            pltpu.VMEM((T, S, F), BF16),
            pltpu.VMEM((1, D), F32),
            pltpu.VMEM((1, D), F32),
            pltpu.VMEM((S, D), BF16),
            pltpu.VMEM((3, D, F), BF16),
            pltpu.VMEM((S, CACHE, F), BF16),
            pltpu.VMEM((S, CACHE, F), BF16),
            pltpu.VMEM((F, D), BF16),
            pltpu.VMEM((books, G, V), BF16),
            pltpu.VMEM((S, CBH, V), F32),
            pltpu.VMEM((S, F), F32),
            pltpu.VMEM((S, F), F32),
            pltpu.VMEM((S, F), F32),
            pltpu.VMEM((S, H, CACHE), F32),
            pltpu.VMEM((S, H, CACHE), F32),
            pltpu.VMEM((S, F), F32),
            pltpu.VMEM((T, S, F), F32),
            pltpu.VMEM((T, S, F), F32),
            pltpu.VMEM((T, 2 * Hs, F), BF16),
            pltpu.VMEM((2 * Hs, D), BF16),
            pltpu.VMEM((Dp, 2 * Hs, G), BF16),
            pltpu.VMEM((Dp, Hs, 128), F32),
            pltpu.VMEM((Dp, 2, CBH, Hs, V), BF16),
            pltpu.VMEM((Dp, 2, CBH, Hs, V), BF16),
            pltpu.VMEM((2, CBH, Hs, V), F32),
            pltpu.VMEM((CBH, Hs, V), F32),
            pltpu.VMEM((CBH, S, V), F32),
            pltpu.VMEM((CBH, S, V), F32),
            pltpu.VMEM((S, 128), F32),
            pltpu.VMEM((T, 8, S), F32),
            dma((20,)),
            dma((T,)), dma((T,)), dma((T,)), dma((T,)), dma((T, 2)), dma((T, 2)),
            dma((Dp,)), dma((Dp,)), dma((Dp,)), dma((Dp,)),
            dma((Dp, 2, CBH)), dma((Dp, 2, CBH)), dma((CBH,)), dma((CBH,)),
            dma((T,)), dma((T,)),
        ],
        compiler_params=pltpu.CompilerParams(
            collective_id=0, has_side_effects=True, vmem_limit_bytes=60 * 1024 * 1024
        ),
    )(
        hidden_in, attn_gain.reshape(1, D), jnp.transpose(w_qkv, (1, 0, 2)), w_out,
        cache_keys, cache_values, cache_len, text_len, final_gain.reshape(1, D), lm_head,
        guidance, uniforms,
    )


def solution(mesh):
    placed = (
        P("cfg", "dp", "tp"),
        P(),
        P(None, None, "tp"),
        P("tp", None),
        P("cfg", "dp", None, "tp"),
        P("cfg", "dp", None, "tp"),
        P("dp"),
        P("dp"),
        P(),
        P(None, "dp", "tp"),
        P("dp"),
        P("dp", "cfg", "tp"),
    )
    return jax.shard_map(
        functools.partial(body, mesh.shape["tp"], mesh.shape["dp"]),
        mesh=mesh,
        in_specs=placed,
        out_specs=(P("dp", "cfg", "tp"), P("cfg", "dp", "tp")),
        check_vma=False,
    )
```
